32 devices in a mesh: replica: 4 (over x, core), fsdp: 8 (over z, y).
Axes of the slice: x: 2, y: 2, z: 4, core: 2. Of those that a mesh axis runs over, the one named last changes fastest.
Arguments:
- anchor: float32 [1536, 1536], P('fsdp', 'replica'), may hold values from -0.15625 to 0.15625
- momentum: float32 [1536, 1536], P('fsdp', 'replica'), may hold values from -0.75 to 0.75
- change: float32 [4, 1536, 1536], P('replica', 'fsdp'), may hold values from -0.75 to 0.75
- adam_first: float32 [4, 1536, 1536], P('replica', 'fsdp'), may hold values from -4 to 4
- adam_second: float32 [4, 1536, 1536], P('replica', 'fsdp'), may hold values from 0.1 to 2
- attn_out: bfloat16 [4, 8192, 1536], P('replica', 'fsdp'), may hold values from -6 to 6
- grad_out: bfloat16 [4, 8192, 1536], P('replica', 'fsdp'), may hold values from -6 to 6
Outputs:
- new_anchor: float32 [1536, 1536], P('fsdp', 'replica')
- new_momentum: float32 [1536, 1536], P('fsdp', 'replica')
- new_local: float32 [4, 1536, 1536], P('replica', 'fsdp')
- new_first: float32 [4, 1536, 1536], P('replica', 'fsdp')
- new_second: float32 [4, 1536, 1536], P('replica', 'fsdp')
- input_grad: bfloat16 [4, 8192, 1536], P('replica', 'fsdp')
The draws below stay inside these ranges and needn't reach their ends.
All inputs are finite; a program needn't handle non-finite values.
Results may differ from the reference program's by a relative error of at most 0.0049.
Values may be sent and summed in bfloat16 or wider, within the bound.
No kernel may reach another device: no remote copies, remote signals or barrier semaphores. Data moves between devices by JAX's collectives and lax.ppermute only.
A program may use at most 128 MiB of HBM per device.

```python
import math
import jax
import jax.numpy as jnp
from jax import lax

D = 1536
REPLICAS = 4
TOKENS = 8192


def spiked(values, key, source, target, shards_of, factor):
    owner, partner = [(jnp.arange(values.shape[dim]) // (values.shape[dim] // shards_of)).reshape([-1 if axis == dim else 1 for axis in range(values.ndim)]) for dim in (source, target)]
    chosen = jax.random.permutation(key, shards_of)[partner]
    strong = (owner == chosen) | (owner == (partner + shards_of // 2) % shards_of)
    return jnp.where(strong, factor * values, values)


def shard_levels(own_key, dims, split, smallest, top_value):
    gain, own = 1.0, jax.random.fold_in(own_key, 6)
    for position, shards_of in split:
        steps = jnp.exp(jax.random.uniform(jax.random.fold_in(own, position), (shards_of,), jnp.float32, smallest / len(split), top_value / len(split)))
        gain = gain * jnp.repeat(steps, dims[position] // shards_of).reshape([-1 if axis == position else 1 for axis in range(len(dims))])
    return gain


def gaussian(own_key, extent, spread, limit, split=(), dtype=jnp.bfloat16):
    result = jax.random.normal(own_key, extent, jnp.float32) * spread
    if len(split) > 0:
        result = shard_levels(own_key, extent, split, -0.22, 0.18) * result
    return jnp.clip(result, min=-limit, max=limit).astype(dtype)


def bell_draw_with(stream_key, extent, deviation, most, cuts, heavy, held_as=jnp.bfloat16):
    result = deviation * jax.random.normal(stream_key, extent, jnp.float32)
    if cuts:
        result = result * shard_levels(stream_key, extent, cuts, -0.22, 0.18)
    return jnp.clip(spiked(result, jax.random.fold_in(stream_key, 3), *heavy), -most, most).astype(held_as)


def setup_inputs(seed: int = 0) -> dict:
    seeds = jax.random.split(jax.random.key(seed), 8)
    return {
        "anchor": gaussian(seeds[0], (D, D), D ** -0.5, 0.15625, ((0, 8), (1, 4)), jnp.float32),
        "momentum": gaussian(seeds[1], (D, D), 0.05, 0.75, ((0, 8), (1, 4)), jnp.float32),
        "change": gaussian(seeds[2], (REPLICAS, D, D), 0.05, 0.75, ((0, 4), (1, 8)), jnp.float32),
        "adam_first": gaussian(seeds[3], (REPLICAS, D, D), 0.3, 4.0, ((0, 4), (1, 8)), jnp.float32),
        "adam_second": jnp.clip(jnp.exp(math.log(2.0) - 2.9957323 * jax.random.uniform(seeds[4], (REPLICAS, D, D), jnp.float32) ** shard_levels(seeds[4], (REPLICAS, D, D), ((0, 4), (1, 8)), -0.2, 0.2)), 0.1, 2.0),
        "attn_out": bell_draw_with(seeds[5], (REPLICAS, TOKENS, D), 1.0, 6.0, ((0, 4), (1, 8)), (1, 2, 8, 2.0)),
        "grad_out": gaussian(seeds[6], (REPLICAS, TOKENS, D), 1.0, 6.0, ((0, 4), (1, 8))),
    }


outer_rate = 0.7
outer_mu = 0.9
inner_rate = 0.005
beta_one = 0.9
beta_two = 0.95
decay_rate = 0.1
epsilon = 1e-08

def reference(anchor, momentum, change, adam_first, adam_second, attn_out, grad_out):
    outer_grad = -lax.optimization_barrier(jnp.sum(change, axis=0)) / REPLICAS
    new_momentum = outer_mu * momentum + outer_grad
    new_anchor = anchor - outer_rate * (outer_grad + outer_mu * new_momentum)
    weights = new_anchor.astype(jnp.bfloat16)
    grad_scale = TOKENS ** (-0.5)

    def one_group(operands):
        inputs, cotangent, first, second = operands
        gradient = jnp.dot(inputs.T, cotangent, preferred_element_type=jnp.float32) * grad_scale
        first_next = beta_one * first + (1.0 - beta_one) * gradient
        second_next = beta_two * second + (1.0 - beta_two) * gradient * gradient
        local = new_anchor - inner_rate * (first_next / (jnp.sqrt(second_next) + epsilon) + decay_rate * new_anchor)
        back = jnp.dot(cotangent, weights.T, preferred_element_type=jnp.float32).astype(jnp.bfloat16)
        return (local, first_next, second_next, back)
    results = lax.map(one_group, (attn_out, grad_out, adam_first, adam_second))
    return (new_anchor, new_momentum, results[0], results[1], results[2], results[3])
```

```python
import jax
import jax.numpy as jnp
from jax import lax
from jax.sharding import PartitionSpec as P

outer_rate = 0.7
outer_mu = 0.9
inner_rate = 0.005
beta_one = 0.9
beta_two = 0.95
decay_rate = 0.1
epsilon = 1e-08

RING_MOST = 8


def ring_of(n):
    order = list(range(0, n, 2)) + list(range(n - 1 - n % 2, 0, -2))
    ahead = [(order[i], order[(i + 1) % n]) for i in range(n)]
    back = [(b, a) for a, b in ahead]
    return order, ahead, back


def reduce_ring(part, at, ahead, back, n):
    rows, width = part.shape[0] // n, part.shape[1]
    cut = width // 2
    far = n // 2

    def own(k, half):
        return lax.dynamic_slice(part, (at(k) * rows, half * cut), (rows, cut))

    def stream(sign, half, hops):
        perm = ahead if sign > 0 else back
        acc = own(sign * hops, half).astype(jnp.bfloat16)
        yield acc
        for k in range(hops - 1, -1, -1):
            acc = lax.ppermute(acc, "fsdp", perm).astype(jnp.float32)
            if k:
                acc = (acc + own(sign * k, half)).astype(jnp.bfloat16)
        yield acc

    def run(sign, half, hops):
        return list(stream(sign, half, hops))[-1]

    near = n - 1 - far
    left = own(0, 0) + run(1, 0, far) + run(-1, 0, near)
    right = own(0, 1) + run(-1, 1, far) + run(1, 1, near)
    return jnp.concatenate([left, right], axis=1)


def gather_ring(block, at, ahead, back, n):
    rows, width = block.shape
    full = jnp.zeros((n * rows, width), block.dtype)
    full = lax.dynamic_update_slice(full, block, (at(0) * rows, 0))
    far = n // 2
    up, down = block, block
    for k in range(1, far + 1):
        up = lax.ppermute(up, "fsdp", ahead)
        full = lax.dynamic_update_slice(full, up, (at(-k) * rows, 0))
        if k < n - far:
            down = lax.ppermute(down, "fsdp", back)
            full = lax.dynamic_update_slice(full, down, (at(k) * rows, 0))
    return full


def swap(value, bit, groups):
    return lax.ppermute(value, "replica", [(r, r ^ bit) for r in range(groups)])


def shards(anchor, momentum, change, adam_first, adam_second, attn_out, grad_out):
    groups = lax.axis_size("replica")
    n = lax.axis_size("fsdp")
    r = lax.axis_index("replica")
    f = lax.axis_index("fsdp")
    order, ahead, back = ring_of(n)
    place = [order.index(i) for i in range(n)]
    p = jnp.array(place, jnp.int32)[f]

    def at(k):
        return jnp.array(order, jnp.int32)[(p + k + n) % n]

    width = anchor.shape[1]
    step_change = change[0]

    def columns(value, q):
        return lax.dynamic_slice_in_dim(value, q * width, width, 1)

    summed = columns(step_change, r)
    for bit in range(1, groups):
        other = columns(step_change, r ^ bit).astype(jnp.bfloat16)
        summed = summed + swap(other, bit, groups).astype(jnp.float32)
    outer_grad = -summed / groups
    new_momentum = outer_mu * momentum + outer_grad
    new_anchor = anchor - outer_rate * (outer_grad + outer_mu * new_momentum)

    inputs = attn_out[0]
    cotangent = grad_out[0]
    part = lax.dot_general(
        inputs, cotangent, (((0,), (0,)), ((), ())), preferred_element_type=jnp.float32
    )
    weights = gather_ring(new_anchor.astype(jnp.bfloat16), at, ahead, back, n)
    pieces = [(0, weights)]
    bit = groups // 2
    while bit:
        pieces = pieces + [(b ^ bit, swap(w, bit, groups)) for b, w in pieces]
        bit //= 2
    total = 0.0
    rows = anchor.shape[0]
    by_column = jnp.zeros((n * rows, groups * width), jnp.bfloat16)
    for b, w in pieces:
        by_column = lax.dynamic_update_slice(by_column, w, (0, (r ^ b) * width))
    input_grad = lax.dot_general(
        cotangent, by_column, (((1,), (1,)), ((), ())), preferred_element_type=jnp.float32
    ).astype(jnp.bfloat16)
    anchor_next = lax.dynamic_slice_in_dim(by_column, f * rows, rows, 0).astype(jnp.float32)

    grad_scale = (inputs.shape[0] * n) ** (-0.5)
    if n <= RING_MOST and n % 2 == 0:
        gradient = reduce_ring(part, at, ahead, back, n)
    else:
        gradient = lax.psum_scatter(part, "fsdp", scatter_dimension=0, tiled=True)
    gradient = gradient * grad_scale
    first_next = beta_one * adam_first[0] + (1.0 - beta_one) * gradient
    second_next = beta_two * adam_second[0] + (1.0 - beta_two) * gradient * gradient
    local = anchor_next - inner_rate * (
        first_next / (jnp.sqrt(second_next) + epsilon) + decay_rate * anchor_next
    )
    return (
        new_anchor,
        new_momentum,
        local[None],
        first_next[None],
        second_next[None],
        input_grad[None],
    )


def solution(mesh):
    in_specs = (
        P("fsdp", "replica"),
        P("fsdp", "replica"),
        P("replica", "fsdp", None),
        P("replica", "fsdp", None),
        P("replica", "fsdp", None),
        P("replica", "fsdp", None),
        P("replica", "fsdp", None),
    )
    out_specs = (
        P("fsdp", "replica"),
        P("fsdp", "replica"),
        P("replica", "fsdp", None),
        P("replica", "fsdp", None),
        P("replica", "fsdp", None),
        P("replica", "fsdp", None),
    )
    return jax.shard_map(shards, mesh=mesh, in_specs=in_specs, out_specs=out_specs, check_vma=False)
```
